32 devices in a mesh: dp: 2 (over z, core), tp: 16 (over x, y).
Axes of the slice: x: 4, y: 4, z: 1, core: 2. Of those that a mesh axis runs over, the one named last changes fastest.
The devices are a block of a 4x4x8 slice.
Arguments:
- x: bfloat16 [128, 2048], P('dp'), parts along dimension 0
- k_cache: bfloat16 [128, 4096, 16, 128], P('dp', None, 'tp'), parts along dimension 0
- v_cache: bfloat16 [128, 4096, 16, 128], P('dp', None, 'tp'), parts along dimension 0
- gain_a: bfloat16 [2048], replicated
- wq: bfloat16 [2048, 2048], P(None, 'tp')
- wo: bfloat16 [2048, 2048], P('tp')
- gain_m: bfloat16 [2048], replicated
- w_gate: bfloat16 [2048, 8192], P(None, 'tp')
- w_up: bfloat16 [2048, 8192], P(None, 'tp')
- w_down: bfloat16 [8192, 2048], P('tp')
Outputs:
- output: bfloat16 [128, 2048], P('dp'), parts along dimension 0
There are 2 independent parts. The reference program is written for one: setup_inputs(seed, part) draws one part's arguments, and reference() takes and returns one part's arrays. A program takes and returns all parts, laid end to end along the dimension named above; an argument that names none is the same for every part.
All inputs are finite; a program needn't handle non-finite values.
Results may differ from the reference program's by a relative error of at most 0.017.
Values are sent between devices in bfloat16 or wider.
A program may use at most 768 MiB of HBM per device.

```python
import jax
import jax.numpy as jnp
from jax import lax

BATCH = 64
CACHE = 4096
D = 2048
HEADS = 16
KV_HEADS = 16
HEAD = 128
FF = 8192
THETA = 10000


def setup_inputs(seed: int = 0, part: int = 0) -> dict:
    kx, kc, kw, kn, kq, ko, km, kg, ku, kd = jax.random.split(jax.random.key(seed), 10)
    kx, kc, kw = (jax.random.fold_in(k, part) for k in (kx, kc, kw))

    def weights(key, rows, columns):
        return jax.random.normal(key, (rows, columns), jnp.float32) * rows**-0.5

    drawn = {
        "x": jax.random.normal(kx, (BATCH, D), jnp.float32),
        "k_cache": 2 * jax.random.normal(kc, (BATCH, CACHE, KV_HEADS, HEAD), jnp.float32),
        "v_cache": 4 * jax.random.normal(kw, (BATCH, CACHE, KV_HEADS, HEAD), jnp.float32),
        "gain_a": 1 + 0.1 * jax.random.normal(kn, (D,), jnp.float32),
        "wq": 2 * weights(kq, D, HEADS * HEAD),
        "wo": weights(ko, HEADS * HEAD, D),
        "gain_m": 1 + 0.1 * jax.random.normal(km, (D,), jnp.float32),
        "w_gate": weights(kg, D, FF),
        "w_up": weights(ku, D, FF),
        "w_down": 2 * weights(kd, FF, D),
    }
    return {k: v.astype(jnp.bfloat16) for k, v in drawn.items()}


def normed(x, gain):
    wide = x.astype(jnp.float32)
    scale = lax.rsqrt(jnp.mean(wide * wide, -1, keepdims=True) + 1e-6)
    return (wide * scale * gain.astype(jnp.float32)).astype(jnp.bfloat16)


def turned(t, place, theta):
    half = t.shape[-1] // 2
    angle = place.astype(jnp.float32)[:, None] * theta ** (-jnp.arange(half, dtype=jnp.float32) / half)
    cos, sin = jnp.cos(angle)[:, None], jnp.sin(angle)[:, None]
    a, b = t[..., :half].astype(jnp.float32), t[..., half:].astype(jnp.float32)
    return jnp.concatenate([a * cos - b * sin, b * cos + a * sin], -1).astype(jnp.bfloat16)


def matmul(a, w):
    return jnp.dot(a, w, preferred_element_type=jnp.float32).astype(jnp.bfloat16)


def einsum(form, a, b):
    return jnp.einsum(form, a.astype(jnp.float32), b.astype(jnp.float32))


def seen_by(a, wq, k_cache, v_cache, head, theta):
    batch, cache, kv_heads = k_cache.shape[:3]
    place = jnp.full((batch,), cache - 1)
    q = turned(matmul(a, wq).reshape(batch, -1, head), place, theta).reshape(batch, kv_heads, -1, head)
    scores = einsum("bgsd,bugd->bgsu", q, k_cache) * head**-0.5
    weights = jax.nn.softmax(scores, -1).astype(jnp.bfloat16)
    return einsum("bgsu,bugd->bgsd", weights, v_cache).astype(jnp.bfloat16).reshape(batch, -1)


def hidden_of(b, w_gate, w_up):
    gate = jnp.dot(b, w_gate, preferred_element_type=jnp.float32)
    up = jnp.dot(b, w_up, preferred_element_type=jnp.float32)
    return (jax.nn.silu(gate) * up).astype(jnp.bfloat16)


def reference(x, k_cache, v_cache, gain_a, wq, wo, gain_m, w_gate, w_up, w_down):
    seen = seen_by(normed(x, gain_a), wq, k_cache, v_cache, HEAD, THETA)
    h = (x.astype(jnp.float32) + jnp.dot(seen, wo, preferred_element_type=jnp.float32)).astype(jnp.bfloat16)
    hidden = hidden_of(normed(h, gain_m), w_gate, w_up)
    return (h.astype(jnp.float32) + jnp.dot(hidden, w_down, preferred_element_type=jnp.float32)).astype(jnp.bfloat16)
```

```python
import functools

import jax
import jax.numpy as jnp
import numpy as np
from jax import lax
from jax.experimental import pallas as pl
from jax.experimental.pallas import tpu as pltpu
from jax.sharding import PartitionSpec as P

HEAD = 128
THETA = 10000
GROUP = 16
PART = 4
SLOTS = 6
BLOCK = 256
UNIT = 8


F32, BF16 = jnp.float32, jnp.bfloat16


def scaled(wide, gain):
    scale = lax.rsqrt(jnp.mean(wide * wide, -1, keepdims=True) + 1e-6)
    return (wide * scale * gain.astype(F32)).astype(BF16)


def dot(a, b):
    return jnp.dot(a, b, preferred_element_type=F32)


def layer(
    side, cache,
    x_hbm, gain_a_hbm, gain_m_hbm, turn_hbm, wq_hbm, wo_hbm, wg_hbm, wu_hbm, wd_hbm, k_hbm, v_hbm,
    y_hbm,
    x_ref, gain_a_ref, gain_m_ref, turn_ref, wq_ref, wo_ref, wg_ref, wu_ref, wd_ref,
    ring, qd, s_ref, p_ref, part_o, h_ref, b_ref, y_ref, first, second,
    in_sem, ring_sem, out_sem, send_sem, recv_sem,
):
    units, _, d = x_ref.shape
    batch = units * UNIT
    half = d // 2
    rows = PART * cache
    per = GROUP // PART
    groups = batch // GROUP
    steps = groups * 2 * per
    me = lax.axis_index("tp")
    mx, my = me // side, me % side
    peers_x = [lax.rem(mx + i, side) * side + my for i in range(1, side)]
    peers_y = [mx * side + lax.rem(my + i, side) for i in range(1, side)]

    barrier = pltpu.get_barrier_semaphore()
    for peer in peers_x + peers_y:
        pl.semaphore_signal(barrier, inc=1, device_id={"tp": peer}, device_id_type=pl.DeviceIdType.MESH)

    def chunk(t, issue):
        g, c = t // (2 * per), t % (2 * per)
        slot = t % SLOTS

        @pl.when(c < per)
        def _():
            copy = pltpu.make_async_copy(k_hbm.at[pl.ds((g * per + c) * rows, rows)], ring.at[slot], ring_sem.at[slot])
            copy.start() if issue else copy.wait()

        @pl.when(c >= per)
        def _():
            copy = pltpu.make_async_copy(v_hbm.at[pl.ds((g * per + c - per) * rows, rows)], ring.at[slot], ring_sem.at[slot])
            copy.start() if issue else copy.wait()

    early = [(x_hbm, x_ref), (gain_a_hbm, gain_a_ref), (gain_m_hbm, gain_m_ref), (turn_hbm, turn_ref), (wq_hbm, wq_ref)]
    late = [(wo_hbm, wo_ref), (wg_hbm, wg_ref), (wu_hbm, wu_ref), (wd_hbm, wd_ref)]
    copies = [pltpu.make_async_copy(a, b, in_sem.at[i]) for i, (a, b) in enumerate(early + late)]
    for copy in copies[:len(early)]:
        copy.start()
    for t in range(SLOTS):
        chunk(t, True)
    for copy in copies[len(early):]:
        copy.start()
    for copy in copies[:len(early)]:
        copy.wait()

    a = scaled(x_ref[...].astype(F32).reshape(batch, d), gain_a_ref[...])
    q = dot(a, wq_ref[...]).astype(BF16).astype(F32)
    q = q * turn_ref[0:1, :] + pltpu.roll(q, HEAD // 2, 1) * turn_ref[1:2, :]
    row = lax.broadcasted_iota(jnp.int32, (GROUP, HEAD), 0)
    for g in range(groups):
        for s in range(GROUP):
            mine = jnp.where(row == s, q[g * GROUP:(g + 1) * GROUP], 0.0).astype(BF16)
            qd[g * per + s // PART, :, (s % PART) * HEAD:(s % PART + 1) * HEAD] = mine
    s_ref[...] = jnp.zeros_like(s_ref)
    pl.semaphore_wait(barrier, 2 * (side - 1))

    def side_by_side(buf, at):
        return jnp.concatenate([buf[pl.ds(i * cache + at, BLOCK), :] for i in range(PART)], axis=1)

    def spread(buf, n, u, hop, along_x, along_y, term):
        for slot, value, peers in ((along_x, term[0], peers_x), (along_y, term[1], peers_y)):
            buf[n, u, slot] = value.astype(BF16)
        for slot, peers in ((along_x, peers_x), (along_y, peers_y)):
            for peer in peers:
                pltpu.make_async_remote_copy(
                    src_ref=buf.at[n, u, slot], dst_ref=buf.at[n, u, slot],
                    send_sem=send_sem.at[n, u, hop], recv_sem=recv_sem.at[n, u, hop],
                    device_id={"tp": peer}, device_id_type=pl.DeviceIdType.MESH,
                ).start()

    def landed(buf, n, u, hop, sem):
        all_of_it = buf.at[n, u, pl.ds(0, 2 * (side - 1))]
        pltpu.make_async_copy(all_of_it, all_of_it, sem.at[n, u, hop]).wait()

    def total(buf, n, u, start):
        t = buf[n, u, start].astype(F32)
        for i in range(1, side):
            t = t + buf[n, u, start + i].astype(F32)
        return t

    def send_terms(n, u, term):
        spread(first, n, u, 0, mx, side + my, (term[:, :half], term[:, half:]))

    def send_sums(n, u):
        landed(first, n, u, 0, recv_sem)
        spread(second, n, u, 1, side + mx, my, (total(first, n, u, side), total(first, n, u, 0)))

    def summed(n, u):
        landed(second, n, u, 1, recv_sem)
        return jnp.concatenate([total(second, n, u, 0), total(second, n, u, side)], axis=1)

    def project(u):
        send_terms(0, u, dot((part_o[0] + part_o[1]).astype(BF16), wo_ref[...]))

    def middle(u):
        h = (x_ref[u].astype(F32) + summed(0, u)).astype(BF16)
        h_ref[u] = h
        b_ref[u] = scaled(h.astype(F32), gain_m_ref[...])

    def mlp(b):
        gate, up = dot(b, wg_ref[...]), dot(b, wu_ref[...])
        return dot((jax.nn.silu(gate) * up).astype(BF16), wd_ref[...])

    def written(u):
        return pltpu.make_async_copy(y_ref.at[u], y_hbm.at[u], out_sem.at[u])

    def finish(u):
        y_ref[u] = (h_ref[u].astype(F32) + summed(1, u)).astype(BF16)
        written(u).start()

    def step(t, carry):
        g, c = t // (2 * per), t % (2 * per)
        slot = t % SLOTS
        chunk(t, False)
        buf = ring.at[slot]

        @pl.when(c < per)
        def _():
            lhs = qd[g * per + c]
            for at in range(0, cache, BLOCK):
                s_ref[:, at:at + BLOCK] += lax.dot_general(
                    lhs, side_by_side(buf, at), (((1,), (1,)), ((), ())), preferred_element_type=F32)

        @pl.when(c >= per)
        def _():
            j = c - per
            acc = jnp.zeros((GROUP, PART * HEAD), F32)
            for at in range(0, cache, BLOCK):
                acc += dot(p_ref[:, at:at + BLOCK], side_by_side(buf, at))
            o = jnp.zeros((GROUP, HEAD), F32)
            for i in range(PART):
                o = jnp.where(row == j * PART + i, acc[:, i * HEAD:(i + 1) * HEAD], o)
            part_o[j % 2] = o[:UNIT] + o[UNIT:]

        @pl.when(t + SLOTS < steps)
        def _():
            chunk(t + SLOTS, True)

        @pl.when(c == per - 1)
        def _():
            scores = s_ref[...] * HEAD**-0.5
            e = jnp.exp(scores - jnp.max(scores, -1, keepdims=True))
            p_ref[...] = (e * (1 / jnp.sum(e, -1, keepdims=True))).astype(BF16)
            s_ref[...] = jnp.zeros_like(s_ref)

        @pl.when(t == per)
        def _():
            for copy in copies[len(early):]:
                copy.wait()

        @pl.when((c == per + 1) | (c == per + 3))
        def _():
            project(2 * g + (c - per) // 2)

        @pl.when((c == 1) & (g > 0))
        def _():
            for i in range(2):
                send_sums(0, 2 * g - 2 + i)

        @pl.when((c == 3) & (g > 0))
        def _():
            for i in range(2):
                middle(2 * g - 2 + i)

        @pl.when((c == 4) & (g > 0))
        def _():
            term = mlp(b_ref[pl.ds(2 * g - 2, 2)].astype(F32).reshape(GROUP, d).astype(BF16))
            for i in range(2):
                send_terms(1, 2 * g - 2 + i, term[i * UNIT:(i + 1) * UNIT])

        @pl.when((c == 7) & (g > 0) & (g < groups - 1))
        def _():
            for i in range(2):
                send_sums(1, 2 * g - 2 + i)

        @pl.when((c == 2) & (g > 1))
        def _():
            for i in range(2):
                finish(2 * g - 4 + i)

        return carry

    lax.fori_loop(0, steps, step, 0)

    e, f = units - 2, units - 1
    send_sums(0, e)
    send_sums(1, e - 2)
    send_sums(1, e - 1)
    send_sums(0, f)
    middle(e)
    send_terms(1, e, mlp(b_ref[e]))
    finish(e - 2)
    finish(e - 1)
    middle(f)
    send_terms(1, f, mlp(b_ref[f]))
    send_sums(1, e)
    send_sums(1, f)
    finish(e)
    finish(f)

    def drain(u, carry):
        written(u).wait()
        for n in range(2):
            landed(first, n, u, 0, send_sem)
            landed(second, n, u, 1, send_sem)
        return carry

    lax.fori_loop(0, units, drain, 0)


def turn_table(cache):
    half = HEAD // 2
    angle = (cache - 1) * float(THETA) ** (-np.arange(half) / half)
    cos, sin = np.cos(angle), np.sin(angle)
    table = np.zeros((8, HEAD), np.float32)
    table[0] = np.concatenate([cos, cos])
    table[1] = np.concatenate([-sin, sin])
    return table


def solution(mesh):
    devices = mesh.shape["tp"]
    side = int(devices**0.5)

    def step(x, k_cache, v_cache, gain_a, wq, wo, gain_m, w_gate, w_up, w_down):
        batch, cache = k_cache.shape[:2]
        d = x.shape[1]
        units = batch // UNIT
        hbm = pl.BlockSpec(memory_space=pltpu.HBM)
        operands = (
            x.reshape(units, UNIT, d), gain_a.reshape(1, d), gain_m.reshape(1, d), turn_table(cache),
            wq, wo, w_gate, w_up, w_down, k_cache.reshape(batch * cache, HEAD), v_cache.reshape(batch * cache, HEAD),
        )
        buffers = pltpu.VMEM((2, units, 2 * side, UNIT, d // 2), BF16)
        y = pl.pallas_call(
            functools.partial(layer, side, cache),
            name="layer",
            out_shape=jax.ShapeDtypeStruct((units, UNIT, d), BF16),
            in_specs=[hbm] * len(operands),
            out_specs=hbm,
            scratch_shapes=[pltpu.VMEM(t.shape, t.dtype) for t in operands[:-2]] + [
                pltpu.VMEM((SLOTS, PART * cache, HEAD), BF16),
                pltpu.VMEM((batch // PART, GROUP, PART * HEAD), BF16),
                pltpu.VMEM((GROUP, cache), F32),
                pltpu.VMEM((GROUP, cache), BF16),
                pltpu.VMEM((2, UNIT, HEAD), F32),
                pltpu.VMEM((units, UNIT, d), BF16),
                pltpu.VMEM((units, UNIT, d), BF16),
                pltpu.VMEM((units, UNIT, d), BF16),
                buffers,
                buffers,
                pltpu.SemaphoreType.DMA((len(operands) - 2,)),
                pltpu.SemaphoreType.DMA((SLOTS,)),
                pltpu.SemaphoreType.DMA((units,)),
                pltpu.SemaphoreType.DMA((2, units, 2)),
                pltpu.SemaphoreType.DMA((2, units, 2)),
            ],
            compiler_params=pltpu.CompilerParams(collective_id=0, has_side_effects=True, vmem_limit_bytes=58 * 2**20),
        )(*operands)
        return y.reshape(batch, d)

    states, cache, columns, rows_of = P("dp", None), P("dp", None, "tp", None), P(None, "tp"), P("tp", None)
    return jax.shard_map(
        step,
        mesh=mesh,
        in_specs=(states, cache, cache, P(None), columns, rows_of, P(None), columns, columns, rows_of),
        out_specs=states,
        check_vma=False,
    )
```

```python
import functools

import jax
import jax.numpy as jnp
import numpy as np
from jax import lax
from jax.experimental import pallas as pl
from jax.experimental.pallas import tpu as pltpu
from jax.sharding import PartitionSpec as P

HEAD = 128
THETA = 10000
PART = 4
CHUNKS = 4
AHEAD = 2
BLOCK = 256
UNIT = 8


F32, BF16 = jnp.float32, jnp.bfloat16


def scaled(wide, gain):
    scale = lax.rsqrt(jnp.mean(wide * wide, -1, keepdims=True) + 1e-6)
    return (wide * scale * gain.astype(F32).reshape(1, -1)).astype(BF16)


def dot(a, b):
    return jnp.dot(a, b, preferred_element_type=F32)


def layer(
    side, cache,
    x_hbm, gain_a_hbm, gain_m_hbm, turn_hbm, wq_hbm, wo_hbm, wg_hbm, wu_hbm, wd_hbm, k_hbm, v_hbm,
    y_ref,
    x_ref, gain_a_ref, gain_m_ref, turn_ref, wq_ref, wo_ref, wg_ref, wu_ref, wd_ref,
    ring, qd, s_ref, p_ref, part_o, h_ref, b_ref, first, second,
    in_sem, ring_sem, send_sem, recv_sem,
):
    units, _, d = x_ref.shape
    batch = units * UNIT
    half = d // 2
    rows = PART * cache
    me = lax.axis_index("tp")
    mx, my = me // side, me % side
    hops = sorted(range(1, side), key=lambda i: -min(i, side - i))
    peers_x = [lax.rem(mx + i, side) * side + my for i in hops]
    peers_y = [mx * side + lax.rem(my + i, side) for i in hops]

    barrier = pltpu.get_barrier_semaphore()
    for peer in peers_x + peers_y:
        pl.semaphore_signal(barrier, inc=1, device_id={"tp": peer}, device_id_type=pl.DeviceIdType.MESH)

    def chunk(u, c):
        slot = lax.rem(u, AHEAD) * CHUNKS + c
        return pltpu.make_async_copy((k_hbm, v_hbm)[c // 2].at[pl.ds((2 * u + c % 2) * rows, rows)], ring.at[slot], ring_sem.at[slot])

    def refill(u, c):
        @pl.when(u + AHEAD < units)
        def _():
            chunk(u + AHEAD, c).start()

    early = [(x_hbm, x_ref), (gain_a_hbm, gain_a_ref), (gain_m_hbm, gain_m_ref), (turn_hbm, turn_ref), (wq_hbm, wq_ref), (wo_hbm, wo_ref)]
    late = [(wg_hbm, wg_ref), (wu_hbm, wu_ref), (wd_hbm, wd_ref)]
    copies = [pltpu.make_async_copy(a, b, in_sem.at[i]) for i, (a, b) in enumerate(early + late)]
    for copy in copies[:len(early) - 1]:
        copy.start()
    for c in range(2):
        chunk(0, c).start()
    for copy in copies[:len(early) - 1]:
        copy.wait()
    copies[len(early) - 1].start()
    for t in range(2, AHEAD * CHUNKS):
        chunk(t // CHUNKS, t % CHUNKS).start()
    for copy in copies[len(early):]:
        copy.start()

    a = scaled(x_ref[...].astype(F32).reshape(batch, d), gain_a_ref[...])
    q = dot(a, wq_ref[...]).astype(BF16).astype(F32)
    q = q * turn_ref[0:1, :] + pltpu.roll(q, HEAD // 2, 1) * turn_ref[1:2, :]
    row = lax.broadcasted_iota(jnp.int32, (UNIT, HEAD), 0)
    for u in range(units):
        for i in range(UNIT):
            qd[u, :, i * HEAD:(i + 1) * HEAD] = jnp.where(row == i, q[u * UNIT:(u + 1) * UNIT], 0.0).astype(BF16)
    pl.semaphore_wait(barrier, 2 * (side - 1))

    def side_by_side(u, chunks, at):
        bufs = [ring.at[lax.rem(u, AHEAD) * CHUNKS + c] for c in chunks]
        return jnp.concatenate([buf[pl.ds(i * cache + at, BLOCK), :] for buf in bufs for i in range(PART)], axis=1)

    def score(u, chunks):
        c = chunks[0] % 2 * PART * HEAD
        lhs = qd[u, :, c:c + len(chunks) * PART * HEAD]
        return [
            lax.dot_general(lhs, side_by_side(u, chunks, at), (((1,), (1,)), ((), ())), preferred_element_type=F32)
            for at in range(0, cache, BLOCK)
        ]

    def weigh():
        scores = s_ref[...] * HEAD**-0.5
        e = jnp.exp(scores - jnp.max(scores, -1, keepdims=True))
        p_ref[...] = (e * (1 / jnp.sum(e, -1, keepdims=True))).astype(BF16)

    def mixed(u, chunks):
        acc = jnp.zeros((UNIT, len(chunks) * PART * HEAD), F32)
        for at in range(0, cache, BLOCK):
            acc += dot(p_ref[:, at:at + BLOCK], side_by_side(u, chunks, at))
        o = jnp.zeros((UNIT, HEAD), F32)
        for i in range(len(chunks) * PART):
            o = jnp.where(row == chunks[0] % 2 * PART + i, acc[:, i * HEAD:(i + 1) * HEAD], o)
        return o

    def spread(buf, n, u, hop, along_x, along_y, term):
        for slot, value, peers in ((along_x, term[0], peers_x), (along_y, term[1], peers_y)):
            buf[n, u, slot] = value.astype(BF16)
        for slot, peers in ((along_x, peers_x), (along_y, peers_y)):
            for peer in peers:
                pltpu.make_async_remote_copy(
                    src_ref=buf.at[n, u, slot], dst_ref=buf.at[n, u, slot],
                    send_sem=send_sem.at[n, u, hop], recv_sem=recv_sem.at[n, u, hop],
                    device_id={"tp": peer}, device_id_type=pl.DeviceIdType.MESH,
                ).start()

    def landed(buf, n, u, hop, sem):
        all_of_it = buf.at[n, u, pl.ds(0, 2 * (side - 1))]
        pltpu.make_async_copy(all_of_it, all_of_it, sem.at[n, u, hop]).wait()

    def total(buf, n, u, start):
        t = buf[n, u, start].astype(F32)
        for i in range(1, side):
            t = t + buf[n, u, start + i].astype(F32)
        return t

    def send_terms(n, u, term):
        spread(first, n, u, 0, mx, side + my, (term[:, :half], term[:, half:]))

    def send_sums(n, u):
        landed(first, n, u, 0, recv_sem)
        spread(second, n, u, 1, side + mx, my, (total(first, n, u, side), total(first, n, u, 0)))

    def summed(n, u):
        landed(second, n, u, 1, recv_sem)
        return jnp.concatenate([total(second, n, u, 0), total(second, n, u, side)], axis=1)

    def project(u, o):
        send_terms(0, u, dot(o.astype(BF16), wo_ref[...]))

    def middle(u):
        h = (x_ref[u].astype(F32) + summed(0, u)).astype(BF16)
        h_ref[u] = h
        b_ref[u] = scaled(h.astype(F32), gain_m_ref[...])

    def mlp(b):
        gate, up = dot(b, wg_ref[...]), dot(b, wu_ref[...])
        return dot((jax.nn.silu(gate) * up).astype(BF16), wd_ref[...])

    def finish(u):
        y_ref[u] = (h_ref[u].astype(F32) + summed(1, u)).astype(BF16)

    def mlp_of_two(u):
        term = mlp(b_ref[pl.ds(u, 2)].astype(F32).reshape(2 * UNIT, d).astype(BF16))
        send_terms(1, u, term[:UNIT])
        send_terms(1, u + 1, term[UNIT:])

    def step(u, carry):
        for c in (0, 1):
            chunk(u, c).wait()
        for i, block in enumerate(score(u, (0, 1))):
            s_ref[:, i * BLOCK:(i + 1) * BLOCK] = block
        for c in (0, 1):
            refill(u, c)
        weigh()

        @pl.when(u == 0)
        def _():
            copies[len(early) - 1].wait()

        @pl.when(u == 2)
        def _():
            for copy in copies[len(early):]:
                copy.wait()

        @pl.when(u == 5)
        def _():
            send_sums(1, u - 5)
            send_sums(1, u - 4)

        for c in (2, 3):
            chunk(u, c).wait()
        project(u, mixed(u, (2, 3)))
        for c in (2, 3):
            refill(u, c)

        @pl.when(u > 0)
        def _():
            send_sums(0, u - 1)

        @pl.when(u == 6)
        def _():
            send_sums(1, u - 4)
            send_sums(1, u - 3)

        @pl.when(u > 1)
        def _():
            middle(u - 2)

        @pl.when((u == 3) | (u == 5))
        def _():
            mlp_of_two(u - 3)

        return carry

    lax.fori_loop(0, units - 1, step, 0)

    e, f = units - 2, units - 1
    for c in (0, 1):
        chunk(f, c).wait()
        for i, block in enumerate(score(f, (c,))):
            at = slice(i * BLOCK, (i + 1) * BLOCK)
            s_ref[:, at] = block + s_ref[:, at] if c else block
    weigh()
    chunk(f, 2).wait()
    part_o[...] = mixed(f, (2,))
    chunk(f, 3).wait()
    project(f, part_o[...] + mixed(f, (3,)))

    def sent(n, u):
        landed(first, n, u, 0, send_sem)
        landed(second, n, u, 1, send_sem)

    def drain(u, carry):
        sent(0, u)
        sent(1, u)
        return carry

    send_sums(0, e)
    middle(e - 1)
    mlp_of_two(e - 2)
    for u in range(e - 4):
        finish(u)
    send_sums(0, f)
    middle(e)
    send_terms(1, e, mlp(b_ref[e]))
    send_sums(1, e - 2)
    send_sums(1, e - 1)
    middle(f)
    send_terms(1, f, mlp(b_ref[f]))
    for u in range(e - 4, e - 2):
        finish(u)
    send_sums(1, e)
    lax.fori_loop(0, e - 2, drain, 0)
    finish(e - 2)
    finish(e - 1)
    send_sums(1, f)
    lax.fori_loop(e - 2, e, drain, 0)
    sent(0, e)
    sent(0, f)
    finish(e)
    sent(1, e)
    finish(f)
    sent(1, f)


def turn_table(cache):
    half = HEAD // 2
    angle = (cache - 1) * float(THETA) ** (-np.arange(half) / half)
    cos, sin = np.cos(angle), np.sin(angle)
    table = np.zeros((8, HEAD), np.float32)
    table[0] = np.concatenate([cos, cos])
    table[1] = np.concatenate([-sin, sin])
    return table


def solution(mesh):
    devices = mesh.shape["tp"]
    side = int(devices**0.5)

    def step(x, k_cache, v_cache, gain_a, wq, wo, gain_m, w_gate, w_up, w_down):
        batch, cache = k_cache.shape[:2]
        d = x.shape[1]
        units = batch // UNIT
        hbm = pl.BlockSpec(memory_space=pltpu.HBM)
        operands = (
            x.reshape(units, UNIT, d), gain_a, gain_m, turn_table(cache),
            wq, wo, w_gate, w_up, w_down, k_cache.reshape(batch * cache, HEAD), v_cache.reshape(batch * cache, HEAD),
        )
        buffers = pltpu.VMEM((2, units, 2 * side, UNIT, d // 2), BF16)
        y = pl.pallas_call(
            functools.partial(layer, side, cache),
            name="layer",
            out_shape=jax.ShapeDtypeStruct((units, UNIT, d), BF16),
            in_specs=[hbm] * len(operands),
            out_specs=pl.BlockSpec(memory_space=pltpu.VMEM),
            scratch_shapes=[pltpu.VMEM(t.shape, t.dtype) for t in operands[:-2]] + [
                pltpu.VMEM((AHEAD * CHUNKS, PART * cache, HEAD), BF16),
                pltpu.VMEM((units, UNIT, UNIT * HEAD), BF16),
                pltpu.VMEM((UNIT, cache), F32),
                pltpu.VMEM((UNIT, cache), BF16),
                pltpu.VMEM((UNIT, HEAD), F32),
                pltpu.VMEM((units, UNIT, d), BF16),
                pltpu.VMEM((units, UNIT, d), BF16),
                buffers,
                buffers,
                pltpu.SemaphoreType.DMA((len(operands) - 2,)),
                pltpu.SemaphoreType.DMA((AHEAD * CHUNKS,)),
                pltpu.SemaphoreType.DMA((2, units, 2)),
                pltpu.SemaphoreType.DMA((2, units, 2)),
            ],
            compiler_params=pltpu.CompilerParams(collective_id=0, has_side_effects=True, vmem_limit_bytes=58 * 2**20),
        )(*operands)
        return y.reshape(batch, d)

    states, cache, columns, rows_of = P("dp", None), P("dp", None, "tp", None), P(None, "tp"), P("tp", None)
    return jax.shard_map(
        step,
        mesh=mesh,
        in_specs=(states, cache, cache, P(None), columns, rows_of, P(None), columns, columns, rows_of),
        out_specs=states,
        check_vma=False,
    )
```

```python
import functools

import jax
import jax.numpy as jnp
import numpy as np
from jax import lax
from jax.experimental import pallas as pl
from jax.experimental.pallas import tpu as pltpu
from jax.sharding import PartitionSpec as P

HEAD = 128
THETA = 10000
PART = 4
CHUNKS = 4
AHEAD = 2
BLOCK = 256
UNIT = 8


F32, BF16 = jnp.float32, jnp.bfloat16


def scaled(wide, gain):
    scale = lax.rsqrt(jnp.mean(wide * wide, -1, keepdims=True) + 1e-6)
    return (wide * scale * gain.astype(F32).reshape(1, -1)).astype(BF16)


def dot(a, b):
    return jnp.dot(a, b, preferred_element_type=F32)


def layer(
    side, cache,
    x_hbm, gain_a_hbm, gain_m_hbm, turn_hbm, wq_hbm, wo_hbm, wg_hbm, wu_hbm, wd_hbm, k_hbm, v_hbm,
    y_ref,
    x_ref, gain_a_ref, gain_m_ref, turn_ref, wq_ref, wo_ref, wg_ref, wu_ref, wd_ref,
    ring, qd, s_ref, p_ref, part_o, h_ref, b_ref, first, second, blocks,
    in_sem, ring_sem, send_sem, recv_sem, block_recv_sem,
):
    units, _, d = x_ref.shape
    batch = units * UNIT
    half = d // 2
    rows = PART * cache
    me = lax.axis_index("tp")
    mx, my = me // side, me % side
    hops = sorted(range(1, side), key=lambda i: -min(i, side - i))
    line_x = [(p, p * side + my) for p in (lax.rem(mx + i, side) for i in hops)]
    line_y = [(p, mx * side + p) for p in (lax.rem(my + i, side) for i in hops)]

    barrier = pltpu.get_barrier_semaphore()
    for _, peer in line_x + line_y:
        pl.semaphore_signal(barrier, inc=1, device_id={"tp": peer}, device_id_type=pl.DeviceIdType.MESH)

    def chunk(u, c):
        turn = lax.rem(u, AHEAD)
        slot = turn * CHUNKS + c
        src = (k_hbm, v_hbm)[c // 2].at[pl.ds((2 * u + c % 2) * rows, rows)]
        return src, ring.at[slot], ring_sem.at[slot], ring_sem.at[AHEAD * CHUNKS + turn]

    def started(u, c):
        src, dst, *sems = chunk(u, c)
        if c < CHUNKS - 1:
            pltpu.make_async_copy(src, dst, sems[0]).start()
            return
        for part in range(2):
            for i in range(PART):
                piece = pl.ds(i * cache + part * cache // 2, cache // 2)
                pltpu.make_async_copy(src.at[piece], dst.at[piece], sems[part]).start()

    def arrived(u, c, parts=(0, 1)):
        src, dst, *sems = chunk(u, c)
        if c < CHUNKS - 1:
            pltpu.make_async_copy(src, dst, sems[0]).wait()
            return
        for part in parts:
            size = pl.ds(0, rows // 2)
            pltpu.make_async_copy(src.at[size], dst.at[size], sems[part]).wait()

    def refill(u, c):
        @pl.when(u + AHEAD < units)
        def _():
            started(u + AHEAD, c)

    early = [(x_hbm, x_ref), (gain_a_hbm, gain_a_ref), (gain_m_hbm, gain_m_ref), (turn_hbm, turn_ref), (wq_hbm, wq_ref), (wo_hbm, wo_ref)]
    late = [(wg_hbm, wg_ref), (wu_hbm, wu_ref), (wd_hbm, wd_ref)]
    copies = [pltpu.make_async_copy(a, b, in_sem.at[i]) for i, (a, b) in enumerate(early + late)]
    for copy in copies[:len(early)]:
        copy.start()
    for c in range(2):
        started(0, c)
    for copy in copies[:len(early) - 1]:
        copy.wait()
    for t in range(2, AHEAD * CHUNKS):
        started(t // CHUNKS, t % CHUNKS)
    for copy in copies[len(early):]:
        copy.start()

    a = scaled(x_ref[...].astype(F32).reshape(batch, d), gain_a_ref[...])
    q = dot(a, wq_ref[...]).astype(BF16).astype(F32)
    q = q * turn_ref[0:1, :] + pltpu.roll(q, HEAD // 2, 1) * turn_ref[1:2, :]
    row = lax.broadcasted_iota(jnp.int32, (UNIT, HEAD), 0)
    for u in range(units):
        for i in range(UNIT):
            qd[u, :, i * HEAD:(i + 1) * HEAD] = jnp.where(row == i, q[u * UNIT:(u + 1) * UNIT], 0.0).astype(BF16)
    pl.semaphore_wait(barrier, 2 * (side - 1))

    def side_by_side(u, c, seqs, at):
        slot = lax.rem(u, AHEAD) * CHUNKS + c
        return jnp.concatenate([ring[slot + i // PART, pl.ds(i % PART * cache + at, BLOCK), :] for i in seqs], axis=1)

    def score(u, seqs):
        lhs = qd[u, :, seqs[0] * HEAD:(seqs[-1] + 1) * HEAD]
        return [
            lax.dot_general(lhs, side_by_side(u, 0, seqs, at), (((1,), (1,)), ((), ())), preferred_element_type=F32)
            for at in range(0, cache, BLOCK)
        ]

    def score_half(u, c):
        arrived(u, c)
        for i, block in enumerate(score(u, range(c * PART, (c + 1) * PART))):
            at = slice(i * BLOCK, (i + 1) * BLOCK)
            s_ref[:, at] = block + s_ref[:, at] if c else block

    def weigh():
        scores = s_ref[...] * HEAD**-0.5
        e = jnp.exp(scores - jnp.max(scores, -1, keepdims=True))
        p_ref[...] = (e * (1 / jnp.sum(e, -1, keepdims=True))).astype(BF16)

    def mixed(u, seqs, start=0, end=cache):
        acc = jnp.zeros((UNIT, len(seqs) * HEAD), F32)
        for at in range(start, end, BLOCK):
            acc += dot(p_ref[:, at:at + BLOCK], side_by_side(u, CHUNKS // 2, seqs, at))
        o = jnp.zeros((UNIT, HEAD), F32)
        for n, i in enumerate(seqs):
            o = jnp.where(row == i, acc[:, n * HEAD:(n + 1) * HEAD], o)
        return o

    def send(src, dst, send_sem, recv_sem, peer):
        pltpu.make_async_remote_copy(
            src_ref=src, dst_ref=dst, send_sem=send_sem, recv_sem=recv_sem,
            device_id={"tp": peer}, device_id_type=pl.DeviceIdType.MESH,
        ).start()

    def landed(slots, sem):
        all_of_it = slots.at[pl.ds(0, 2 * (side - 1))]
        pltpu.make_async_copy(all_of_it, all_of_it, sem).wait()

    def total(slots, start):
        t = slots[start].astype(F32)
        for i in range(1, side):
            t = t + slots[start + i].astype(F32)
        return t

    def spread(slots, sems, along_x, along_y, term):
        for slot, value in ((along_x, term[0]), (along_y, term[1])):
            slots[slot] = value.astype(BF16)
        for slot, line in ((along_x, line_x), (along_y, line_y)):
            for _, peer in line:
                send(slots.at[slot], slots.at[slot], *sems, peer)

    def sems(u, hop):
        return send_sem.at[hop], recv_sem.at[u, hop]

    def send_terms(u, term):
        spread(first.at[u], sems(u, 0), mx, side + my, (term[:, :half], term[:, half:]))

    def send_sums(u):
        landed(first.at[u], recv_sem.at[u, 0])
        spread(second.at[u], sems(u, 1), side + mx, my, (total(first.at[u], side), total(first.at[u], 0)))

    def summed(u):
        landed(second.at[u], recv_sem.at[u, 1])
        return jnp.concatenate([total(second.at[u], 0), total(second.at[u], side)], axis=1)

    def block_sems(u, hop):
        return send_sem.at[2], block_recv_sem.at[u, hop]

    def scatter(u, term):
        width = half // side
        out, slots = blocks.at[0, u], blocks.at[1, u]
        for i in range(2 * side):
            out[i] = term[:, i * width:(i + 1) * width].astype(BF16)
        for start, mine, line in ((0, mx, line_x), (side, my, line_y)):
            slots[start + mine] = out[start + mine]
            for p, peer in line:
                send(out.at[start + p], slots.at[start + mine], *block_sems(u, 0), peer)

    def across(u):
        slots = blocks.at[1, u]
        landed(slots, block_recv_sem.at[u, 0])
        spread(blocks.at[2, u], block_sems(u, 1), side + mx, my, (total(slots, side), total(slots, 0)))

    def gather(u):
        slots = blocks.at[2, u]
        landed(slots, block_recv_sem.at[u, 1])
        spread(blocks.at[3, u], block_sems(u, 2), mx, side + my, (total(slots, 0), total(slots, side)))

    def gathered(u):
        slots = blocks.at[3, u]
        landed(slots, block_recv_sem.at[u, 2])
        return jnp.concatenate([slots[i].astype(F32) for i in range(2 * side)], axis=1)

    def project(u, o):
        send_terms(u, dot(o.astype(BF16), wo_ref[...]))

    def middle(u):
        h = (x_ref[u].astype(F32) + summed(u)).astype(BF16)
        h_ref[u] = h
        b_ref[u] = scaled(h.astype(F32), gain_m_ref[...])

    def mlp(b):
        gate, up = dot(b, wg_ref[...]), dot(b, wu_ref[...])
        return dot((jax.nn.silu(gate) * up).astype(BF16), wd_ref[...])

    def finish(u, total):
        y_ref[u] = (h_ref[u].astype(F32) + total).astype(BF16)

    def mlp_of(u, n):
        term = mlp(b_ref[pl.ds(u, n)].astype(F32).reshape(n * UNIT, d).astype(BF16))
        for i in range(n):
            scatter(u + i, term[i * UNIT:(i + 1) * UNIT])

    def step(u, carry):
        for c in (0, 1):
            score_half(u, c)
            refill(u, c)
        weigh()

        @pl.when(u == 0)
        def _():
            copies[len(early) - 1].wait()

        @pl.when(u == 2)
        def _():
            for copy in copies[len(early):]:
                copy.wait()

        arrived(u, 2)
        part_o[...] = mixed(u, range(PART))
        refill(u, 2)
        arrived(u, 3)
        project(u, part_o[...] + mixed(u, range(PART, UNIT)))
        refill(u, 3)

        @pl.when(u > 0)
        def _():
            send_sums(u - 1)

        @pl.when((u > 1) & (u < units - 2))
        def _():
            middle(u - 2)

        @pl.when(u == 3)
        def _():
            mlp_of(u - 3, 2)

        return carry

    lax.fori_loop(0, units - 1, step, 0)

    e, f = units - 2, units - 1
    for c in (0, 1):
        score_half(f, c)
    weigh()
    arrived(f, 2)
    part_o[...] = mixed(f, range(PART))
    arrived(f, 3, (0,))
    part_o[...] += mixed(f, range(PART, UNIT), 0, cache // 2)
    arrived(f, 3, (1,))
    project(f, part_o[...] + mixed(f, range(PART, UNIT), cache // 2, cache))

    send_sums(e)
    middle(e - 2)
    middle(e - 1)
    mlp_of(e - 4, 4)
    send_sums(f)
    middle(e)
    scatter(e, mlp(b_ref[e]))
    for u in range(e):
        across(u)
    middle(f)
    send_terms(units, mlp(b_ref[f]))
    across(e)
    for u in range(e):
        gather(u)
    send_sums(units)
    gather(e)
    for u in range(e):
        finish(u, gathered(u))
    finish(f, summed(units))
    finish(e, gathered(e))

    others = pl.ds(0, 2 * (side - 1))
    for sem, sent in enumerate((first.at[:, others], second.at[:, others], blocks.at[pl.ds(0, 3), :, others])):
        pltpu.make_async_copy(sent, sent, send_sem.at[sem]).wait()


def turn_table(cache):
    half = HEAD // 2
    angle = (cache - 1) * float(THETA) ** (-np.arange(half) / half)
    cos, sin = np.cos(angle), np.sin(angle)
    table = np.zeros((8, HEAD), np.float32)
    table[0] = np.concatenate([cos, cos])
    table[1] = np.concatenate([-sin, sin])
    return table


def solution(mesh):
    devices = mesh.shape["tp"]
    side = int(devices**0.5)

    def step(x, k_cache, v_cache, gain_a, wq, wo, gain_m, w_gate, w_up, w_down):
        batch, cache = k_cache.shape[:2]
        d = x.shape[1]
        units = batch // UNIT
        hbm = pl.BlockSpec(memory_space=pltpu.HBM)
        operands = (
            x.reshape(units, UNIT, d), gain_a, gain_m, jnp.asarray(turn_table(cache)),
            wq, wo, w_gate, w_up, w_down, k_cache.reshape(batch * cache, HEAD), v_cache.reshape(batch * cache, HEAD),
        )
        operands = tuple(pltpu.with_memory_space_constraint(t, pltpu.HBM) for t in operands)
        buffers = pltpu.VMEM((units + 1, 2 * side, UNIT, d // 2), BF16)
        y = pl.pallas_call(
            functools.partial(layer, side, cache),
            name="layer",
            out_shape=jax.ShapeDtypeStruct((units, UNIT, d), BF16),
            in_specs=[hbm] * len(operands),
            out_specs=pl.BlockSpec(memory_space=pltpu.VMEM),
            scratch_shapes=[pltpu.VMEM(t.shape, t.dtype) for t in operands[:-2]] + [
                pltpu.VMEM((AHEAD * CHUNKS, PART * cache, HEAD), BF16),
                pltpu.VMEM((units, UNIT, UNIT * HEAD), BF16),
                pltpu.VMEM((UNIT, cache), F32),
                pltpu.VMEM((UNIT, cache), BF16),
                pltpu.VMEM((UNIT, HEAD), F32),
                pltpu.VMEM((units, UNIT, d), BF16),
                pltpu.VMEM((units, UNIT, d), BF16),
                buffers,
                buffers,
                pltpu.VMEM((4, units - 1, 2 * side, UNIT, d // 2 // side), BF16),
                pltpu.SemaphoreType.DMA((len(operands) - 2,)),
                pltpu.SemaphoreType.DMA((AHEAD * (CHUNKS + 1),)),
                pltpu.SemaphoreType.DMA((3,)),
                pltpu.SemaphoreType.DMA((units + 1, 2)),
                pltpu.SemaphoreType.DMA((units - 1, 3)),
            ],
            compiler_params=pltpu.CompilerParams(collective_id=0, has_side_effects=True, vmem_limit_bytes=52 * 2**20),
        )(*operands)
        return y.reshape(batch, d)

    states, cache, columns, rows_of = P("dp", None), P("dp", None, "tp", None), P(None, "tp"), P("tp", None)
    return jax.shard_map(
        step,
        mesh=mesh,
        in_specs=(states, cache, cache, P(None), columns, rows_of, P(None), columns, columns, rows_of),
        out_specs=states,
        check_vma=False,
    )
```

```python
import functools

import jax
import jax.numpy as jnp
import numpy as np
from jax import lax
from jax.experimental import pallas as pl
from jax.experimental.pallas import tpu as pltpu
from jax.sharding import PartitionSpec as P

HEAD = 128
THETA = 10000
PART = 4
CHUNKS = 4
AHEAD = 2
BLOCK = 256
UNIT = 8


F32, BF16 = jnp.float32, jnp.bfloat16


def scaled(wide, gain):
    scale = lax.rsqrt(jnp.mean(wide * wide, -1, keepdims=True) + 1e-6)
    return (wide * scale * gain.astype(F32).reshape(1, -1)).astype(BF16)


def dot(a, b):
    return jnp.dot(a, b, preferred_element_type=F32)


def layer(
    side, cache,
    x_hbm, gain_a_hbm, gain_m_hbm, turn_hbm, wq_hbm, wo_hbm, wg_hbm, wu_hbm, wd_hbm, k_hbm, v_hbm,
    y_ref,
    x_ref, gain_a_ref, gain_m_ref, turn_ref, wq_ref, wo_ref, wg_ref, wu_ref, wd_ref,
    ring, qd, s_ref, p_ref, part_o, h_ref, b_ref, first, second, dealt,
    in_sem, ring_sem, send_sem, recv_sem, deal_recv_sem,
):
    units, _, d = x_ref.shape
    batch = units * UNIT
    half = d // 2
    rows = PART * cache
    me = lax.axis_index("tp")
    mx, my = me // side, me % side
    hops = sorted(range(1, side), key=lambda i: -min(i, side - i))
    line_x = [lax.rem(mx + i, side) * side + my for i in hops]
    line_y = [mx * side + lax.rem(my + i, side) for i in hops]

    barrier = pltpu.get_barrier_semaphore()
    everyone = sorted(((i, j) for i in range(side) for j in range(side)), key=lambda t: -sum(min(i, side - i) for i in t))[:-1]
    everyone = [lax.rem(mx + i, side) * side + lax.rem(my + j, side) for i, j in everyone]
    for peer in everyone:
        pl.semaphore_signal(barrier, inc=1, device_id={"tp": peer}, device_id_type=pl.DeviceIdType.MESH)

    def chunk(u, c):
        turn = lax.rem(u, AHEAD)
        slot = turn * CHUNKS + c
        src = (k_hbm, v_hbm)[c // 2].at[pl.ds((2 * u + c % 2) * rows, rows)]
        return src, ring.at[slot], ring_sem.at[slot], ring_sem.at[AHEAD * CHUNKS + turn]

    def started(u, c):
        src, dst, *sems = chunk(u, c)
        if c < CHUNKS - 1:
            pltpu.make_async_copy(src, dst, sems[0]).start()
            return
        for part in range(2):
            for i in range(PART):
                piece = pl.ds(i * cache + part * cache // 2, cache // 2)
                pltpu.make_async_copy(src.at[piece], dst.at[piece], sems[part]).start()

    def arrived(u, c, parts=(0, 1)):
        src, dst, *sems = chunk(u, c)
        if c < CHUNKS - 1:
            pltpu.make_async_copy(src, dst, sems[0]).wait()
            return
        for part in parts:
            size = pl.ds(0, rows // 2)
            pltpu.make_async_copy(src.at[size], dst.at[size], sems[part]).wait()

    def refill(u, c):
        @pl.when(u + AHEAD < units)
        def _():
            started(u + AHEAD, c)

    early = [(x_hbm, x_ref), (gain_a_hbm, gain_a_ref), (gain_m_hbm, gain_m_ref), (turn_hbm, turn_ref), (wq_hbm, wq_ref), (wo_hbm, wo_ref)]
    late = [(wg_hbm, wg_ref), (wu_hbm, wu_ref), (wd_hbm, wd_ref)]
    copies = [pltpu.make_async_copy(a, b, in_sem.at[i]) for i, (a, b) in enumerate(early + late)]
    for copy in copies[:len(early)]:
        copy.start()
    for c in range(2):
        started(0, c)
    for copy in copies[:len(early) - 1]:
        copy.wait()
    for t in range(2, AHEAD * CHUNKS):
        started(t // CHUNKS, t % CHUNKS)

    a = scaled(x_ref[...].astype(F32).reshape(batch, d), gain_a_ref[...])
    q = dot(a, wq_ref[...]).astype(BF16).astype(F32)
    q = q * turn_ref[0:1, :] + pltpu.roll(q, HEAD // 2, 1) * turn_ref[1:2, :]
    row = lax.broadcasted_iota(jnp.int32, (UNIT, HEAD), 0)
    for u in range(units):
        for i in range(UNIT):
            qd[u, :, i * HEAD:(i + 1) * HEAD] = jnp.where(row == i, q[u * UNIT:(u + 1) * UNIT], 0.0).astype(BF16)
    pl.semaphore_wait(barrier, len(everyone))

    def side_by_side(u, c, seqs, at):
        slot = lax.rem(u, AHEAD) * CHUNKS + c
        return jnp.concatenate([ring[slot + i // PART, pl.ds(i % PART * cache + at, BLOCK), :] for i in seqs], axis=1)

    def score(u, seqs):
        lhs = qd[u, :, seqs[0] * HEAD:(seqs[-1] + 1) * HEAD]
        return [
            lax.dot_general(lhs, side_by_side(u, 0, seqs, at), (((1,), (1,)), ((), ())), preferred_element_type=F32)
            for at in range(0, cache, BLOCK)
        ]

    def score_half(u, c):
        arrived(u, c)
        for i, block in enumerate(score(u, range(c * PART, (c + 1) * PART))):
            at = slice(i * BLOCK, (i + 1) * BLOCK)
            s_ref[:, at] = block + s_ref[:, at] if c else block

    def weigh():
        scores = s_ref[...] * HEAD**-0.5
        e = jnp.exp(scores - jnp.max(scores, -1, keepdims=True))
        p_ref[...] = (e * (1 / jnp.sum(e, -1, keepdims=True))).astype(BF16)

    def mixed(u, seqs, start=0, end=cache):
        acc = jnp.zeros((UNIT, len(seqs) * HEAD), F32)
        for at in range(start, end, BLOCK):
            acc += dot(p_ref[:, at:at + BLOCK], side_by_side(u, CHUNKS // 2, seqs, at))
        o = jnp.zeros((UNIT, HEAD), F32)
        for n, i in enumerate(seqs):
            o = jnp.where(row == i, acc[:, n * HEAD:(n + 1) * HEAD], o)
        return o

    def send(src, dst, send_sem, recv_sem, peer):
        pltpu.make_async_remote_copy(
            src_ref=src, dst_ref=dst, send_sem=send_sem, recv_sem=recv_sem,
            device_id={"tp": peer}, device_id_type=pl.DeviceIdType.MESH,
        ).start()

    def landed(slots, sem):
        all_of_it = slots.at[pl.ds(0, 2 * (side - 1))]
        pltpu.make_async_copy(all_of_it, all_of_it, sem).wait()

    def total(slots, start):
        t = slots[start].astype(F32)
        for i in range(1, side):
            t = t + slots[start + i].astype(F32)
        return t

    def spread(slots, sems, along_x, along_y, term):
        for slot, value in ((along_x, term[0]), (along_y, term[1])):
            slots[slot] = value.astype(BF16)
        for slot, line in ((along_x, line_x), (along_y, line_y)):
            for peer in line:
                send(slots.at[slot], slots.at[slot], *sems, peer)

    def sems(u, hop):
        return send_sem.at[hop], recv_sem.at[u, hop]

    def send_terms(u, term):
        spread(first.at[u], sems(u, 0), mx, side + my, (term[:, :half], term[:, half:]))

    def send_sums(u):
        landed(first.at[u], recv_sem.at[u, 0])
        spread(second.at[u], sems(u, 1), side + mx, my, (total(first.at[u], side), total(first.at[u], 0)))

    def summed(u):
        landed(second.at[u], recv_sem.at[u, 1])
        return jnp.concatenate([total(second.at[u], 0), total(second.at[u], side)], axis=1)

    def deal():
        slots = dealt.at[1]
        slots[me] = dealt[0, me]
        for peer in everyone:
            send(dealt.at[0, peer], slots.at[me], send_sem.at[2], deal_recv_sem.at[0], peer)

    def waited(slots, sem):
        rest = slots.at[pl.ds(0, side * side - 1)]
        pltpu.make_async_copy(rest, rest, sem).wait()

    def settle():
        slots, sums = dealt.at[1], dealt.at[2]
        waited(slots, deal_recv_sem.at[0])
        t = slots[0].astype(F32)
        for i in range(1, side * side):
            t = t + slots[i].astype(F32)
        sums[me] = t.astype(BF16)
        for peer in everyone:
            send(sums.at[me], sums.at[me], send_sem.at[3], deal_recv_sem.at[1], peer)

    def settled():
        sums = dealt.at[2]
        waited(sums, deal_recv_sem.at[1])
        return jnp.concatenate([sums[i].astype(F32) for i in range(side * side)], axis=1)

    def project(u, o):
        send_terms(u, dot(o.astype(BF16), wo_ref[...]))

    def middle(u):
        h = (x_ref[u].astype(F32) + summed(u)).astype(BF16)
        h_ref[u] = h
        b_ref[u] = scaled(h.astype(F32), gain_m_ref[...])

    def mlp(b):
        gate, up = dot(b, wg_ref[...]), dot(b, wu_ref[...])
        return dot((jax.nn.silu(gate) * up).astype(BF16), wd_ref[...])

    def finish(u, total):
        y_ref[u] = (h_ref[u].astype(F32) + total).astype(BF16)

    def step(u, carry):
        for c in (0, 1):
            score_half(u, c)
            refill(u, c)
        weigh()

        @pl.when(u == 0)
        def _():
            copies[len(early) - 1].wait()

        arrived(u, 2)
        part_o[...] = mixed(u, range(PART))
        refill(u, 2)
        arrived(u, 3)
        project(u, part_o[...] + mixed(u, range(PART, UNIT)))
        refill(u, 3)

        @pl.when(u > 0)
        def _():
            send_sums(u - 1)

        @pl.when((u > 1) & (u < units - 2))
        def _():
            middle(u - 2)

        return carry

    lax.fori_loop(0, units - 1, step, 0)

    e, f = units - 2, units - 1
    for c in (0, 1):
        score_half(f, c)
    weigh()
    arrived(f, 2)
    part_o[...] = mixed(f, range(PART))
    arrived(f, 3, (0,))
    part_o[...] += mixed(f, range(PART, UNIT), 0, cache // 2)
    arrived(f, 3, (1,))
    for copy in copies[len(early):]:
        copy.start()
    project(f, part_o[...] + mixed(f, range(PART, UNIT), cache // 2, cache))

    send_sums(e)
    middle(e - 2)
    middle(e - 1)
    for copy in copies[len(early):]:
        copy.wait()
    term = mlp(b_ref[pl.ds(0, e)].astype(F32).reshape(e * UNIT, d).astype(BF16))
    width = d // (side * side)
    for i in range(side * side):
        dealt[0, i] = term[:, i * width:(i + 1) * width].astype(BF16)
    send_sums(f)
    deal()
    middle(e)
    send_terms(units, mlp(b_ref[e]))
    middle(f)
    send_terms(units + 1, mlp(b_ref[f]))
    settle()
    send_sums(units)
    send_sums(units + 1)
    finish(e, summed(units))
    t = settled()
    for u in range(e):
        finish(u, t[u * UNIT:(u + 1) * UNIT])
    finish(f, summed(units + 1))

    others, rest = pl.ds(0, 2 * (side - 1)), pl.ds(0, side * side - 1)
    for sem, sent in enumerate((first.at[:, others], second.at[:, others], dealt.at[0, rest], dealt.at[2, rest])):
        pltpu.make_async_copy(sent, sent, send_sem.at[sem]).wait()


def turn_table(cache):
    half = HEAD // 2
    angle = (cache - 1) * float(THETA) ** (-np.arange(half) / half)
    cos, sin = np.cos(angle), np.sin(angle)
    table = np.zeros((8, HEAD), np.float32)
    table[0] = np.concatenate([cos, cos])
    table[1] = np.concatenate([-sin, sin])
    return table


def solution(mesh):
    devices = mesh.shape["tp"]
    side = int(devices**0.5)

    def step(x, k_cache, v_cache, gain_a, wq, wo, gain_m, w_gate, w_up, w_down):
        batch, cache = k_cache.shape[:2]
        d = x.shape[1]
        units = batch // UNIT
        hbm = pl.BlockSpec(memory_space=pltpu.HBM)
        operands = (
            x.reshape(units, UNIT, d), gain_a, gain_m, jnp.asarray(turn_table(cache)),
            wq, wo, w_gate, w_up, w_down, k_cache.reshape(batch * cache, HEAD), v_cache.reshape(batch * cache, HEAD),
        )
        operands = tuple(pltpu.with_memory_space_constraint(t, pltpu.HBM) for t in operands)
        buffers = pltpu.VMEM((units + 2, 2 * side, UNIT, d // 2), BF16)
        y = pl.pallas_call(
            functools.partial(layer, side, cache),
            name="layer",
            out_shape=jax.ShapeDtypeStruct((units, UNIT, d), BF16),
            in_specs=[hbm] * len(operands),
            out_specs=pl.BlockSpec(memory_space=pltpu.VMEM),
            scratch_shapes=[pltpu.VMEM(t.shape, t.dtype) for t in operands[:-2]] + [
                pltpu.VMEM((AHEAD * CHUNKS, PART * cache, HEAD), BF16),
                pltpu.VMEM((units, UNIT, UNIT * HEAD), BF16),
                pltpu.VMEM((UNIT, cache), F32),
                pltpu.VMEM((UNIT, cache), BF16),
                pltpu.VMEM((UNIT, HEAD), F32),
                pltpu.VMEM((units, UNIT, d), BF16),
                pltpu.VMEM((units, UNIT, d), BF16),
                buffers,
                buffers,
                pltpu.VMEM((3, devices, (units - 2) * UNIT, d // devices), BF16),
                pltpu.SemaphoreType.DMA((len(operands) - 2,)),
                pltpu.SemaphoreType.DMA((AHEAD * (CHUNKS + 1),)),
                pltpu.SemaphoreType.DMA((4,)),
                pltpu.SemaphoreType.DMA((units + 2, 2)),
                pltpu.SemaphoreType.DMA((2,)),
            ],
            compiler_params=pltpu.CompilerParams(collective_id=0, has_side_effects=True, vmem_limit_bytes=52 * 2**20),
        )(*operands)
        return y.reshape(batch, d)

    states, cache, columns, rows_of = P("dp", None), P("dp", None, "tp", None), P(None, "tp"), P("tp", None)
    return jax.shard_map(
        step,
        mesh=mesh,
        in_specs=(states, cache, cache, P(None), columns, rows_of, P(None), columns, columns, rows_of),
        out_specs=states,
        check_vma=False,
    )
```

```python
import functools

import jax
import jax.numpy as jnp
import numpy as np
from jax import lax
from jax.experimental import pallas as pl
from jax.experimental.pallas import tpu as pltpu
from jax.sharding import PartitionSpec as P

HEAD = 128
THETA = 10000
PART = 4
CHUNKS = 4
TURNS = 4
AHEAD = 2
BLOCK = 256
UNIT = 8


F32, BF16 = jnp.float32, jnp.bfloat16


def scaled(wide, gain):
    scale = lax.rsqrt(jnp.mean(wide * wide, -1, keepdims=True) + 1e-6)
    return (wide * scale * gain.astype(F32).reshape(1, -1)).astype(BF16)


def dot(a, b):
    return jnp.dot(a, b, preferred_element_type=F32)


def layer(
    side, cache,
    x_hbm, gain_a_hbm, gain_m_hbm, turn_hbm, wq_hbm, wo_hbm, wg_hbm, wu_hbm, wd_hbm, k_hbm, v_hbm,
    y_ref,
    x_ref, gain_a_ref, gain_m_ref, turn_ref, wq_ref, wo_ref, wg_ref, wu_ref, wd_ref,
    ring, qd, s_ref, p_ref, part_o, h_ref, b_ref, first, second, dealt,
    in_sem, ring_sem, send_sem, recv_sem, deal_recv_sem,
):
    units, _, d = x_ref.shape
    batch = units * UNIT
    half = d // 2
    rows = PART * cache
    me = lax.axis_index("tp")
    mx, my = me // side, me % side
    hops = sorted(range(1, side), key=lambda i: -min(i, side - i))
    line_x = [lax.rem(mx + i, side) * side + my for i in hops]
    line_y = [mx * side + lax.rem(my + i, side) for i in hops]

    barrier = pltpu.get_barrier_semaphore()
    everyone = sorted(((i, j) for i in range(side) for j in range(side)), key=lambda t: -sum(min(i, side - i) for i in t))[:-1]
    everyone = [lax.rem(mx + i, side) * side + lax.rem(my + j, side) for i, j in everyone]
    for peer in everyone:
        pl.semaphore_signal(barrier, inc=1, device_id={"tp": peer}, device_id_type=pl.DeviceIdType.MESH)

    def chunk(u, c):
        turn = lax.rem(u, AHEAD)
        slot = turn * CHUNKS + c
        src = (k_hbm, v_hbm)[c // 2].at[pl.ds((2 * u + c % 2) * rows, rows)]
        return src, ring.at[slot], ring_sem.at[slot], ring_sem.at[AHEAD * CHUNKS + turn]

    def started(u, c):
        src, dst, *sems = chunk(u, c)
        if c < CHUNKS - 1:
            pltpu.make_async_copy(src, dst, sems[0]).start()
            return
        for part in range(2):
            for i in range(PART):
                piece = pl.ds(i * cache + part * cache // 2, cache // 2)
                pltpu.make_async_copy(src.at[piece], dst.at[piece], sems[part]).start()

    def arrived(u, c, parts=(0, 1)):
        src, dst, *sems = chunk(u, c)
        if c < CHUNKS - 1:
            pltpu.make_async_copy(src, dst, sems[0]).wait()
            return
        for part in parts:
            size = pl.ds(0, rows // 2)
            pltpu.make_async_copy(src.at[size], dst.at[size], sems[part]).wait()

    def refill(u, c):
        @pl.when(u + AHEAD < units)
        def _():
            started(u + AHEAD, c)

    early = [(x_hbm, x_ref), (gain_a_hbm, gain_a_ref), (gain_m_hbm, gain_m_ref), (turn_hbm, turn_ref), (wq_hbm, wq_ref), (wo_hbm, wo_ref)]
    late = [(wg_hbm, wg_ref), (wu_hbm, wu_ref), (wd_hbm, wd_ref)]
    in_sems = [ring_sem.at[2 + i] for i in range(len(early) - 1)] + [in_sem.at[i] for i in range(len(late) + 1)]
    copies = [pltpu.make_async_copy(a, b, sem) for (a, b), sem in zip(early + late, in_sems)]
    for copy in copies[:len(early)]:
        copy.start()
    for c in range(2):
        started(0, c)
    for copy in copies[:len(early) - 1]:
        copy.wait()
    for t in range(2, AHEAD * CHUNKS):
        started(t // CHUNKS, t % CHUNKS)

    a = scaled(x_ref[...].astype(F32).reshape(batch, d), gain_a_ref[...])
    q = dot(a, wq_ref[...]).astype(BF16).astype(F32)
    q = q * turn_ref[0:1, :] + pltpu.roll(q, HEAD // 2, 1) * turn_ref[1:2, :]
    row = lax.broadcasted_iota(jnp.int32, (UNIT, HEAD), 0)
    for u in range(units):
        for i in range(UNIT):
            qd[u, :, i * HEAD:(i + 1) * HEAD] = jnp.where(row == i, q[u * UNIT:(u + 1) * UNIT], 0.0).astype(BF16)
    pl.semaphore_wait(barrier, len(everyone))

    def side_by_side(u, c, seqs, at):
        slot = lax.rem(u, AHEAD) * CHUNKS + c
        return jnp.concatenate([ring[slot + i // PART, pl.ds(i % PART * cache + at, BLOCK), :] for i in seqs], axis=1)

    def score(u, seqs):
        lhs = qd[u, :, seqs[0] * HEAD:(seqs[-1] + 1) * HEAD]
        return [
            lax.dot_general(lhs, side_by_side(u, 0, seqs, at), (((1,), (1,)), ((), ())), preferred_element_type=F32)
            for at in range(0, cache, BLOCK)
        ]

    def score_half(u, c):
        arrived(u, c)
        for i, block in enumerate(score(u, range(c * PART, (c + 1) * PART))):
            at = slice(i * BLOCK, (i + 1) * BLOCK)
            s_ref[:, at] = block + s_ref[:, at] if c else block

    def weigh():
        scores = s_ref[...] * HEAD**-0.5
        e = jnp.exp(scores - jnp.max(scores, -1, keepdims=True))
        p_ref[...] = (e * (1 / jnp.sum(e, -1, keepdims=True))).astype(BF16)

    def mixed(u, seqs, start=0, end=cache):
        acc = jnp.zeros((UNIT, len(seqs) * HEAD), F32)
        for at in range(start, end, BLOCK):
            acc += dot(p_ref[:, at:at + BLOCK], side_by_side(u, CHUNKS // 2, seqs, at))
        o = jnp.zeros((UNIT, HEAD), F32)
        for n, i in enumerate(seqs):
            o = jnp.where(row == i, acc[:, n * HEAD:(n + 1) * HEAD], o)
        return o

    def send(src, dst, send_sem, recv_sem, peer):
        pltpu.make_async_remote_copy(
            src_ref=src, dst_ref=dst, send_sem=send_sem, recv_sem=recv_sem,
            device_id={"tp": peer}, device_id_type=pl.DeviceIdType.MESH,
        ).start()

    def landed(slots, sem):
        all_of_it = slots.at[pl.ds(0, 2 * (side - 1))]
        pltpu.make_async_copy(all_of_it, all_of_it, sem).wait()

    def total(slots, start):
        t = slots[start].astype(F32)
        for i in range(1, side):
            t = t + slots[start + i].astype(F32)
        return t

    def spread(slots, sems, along_x, along_y, term):
        for slot, value in ((along_x, term[0]), (along_y, term[1])):
            slots[slot] = value.astype(BF16)
        for slot, line in ((along_x, line_x), (along_y, line_y)):
            for peer in line:
                send(slots.at[slot], slots.at[slot], *sems, peer)

    def turn(u):
        return u - units + TURNS if isinstance(u, int) and u >= units else lax.rem(u, TURNS)

    def sems(u, hop):
        return send_sem.at[hop], recv_sem.at[turn(u), hop]

    def send_terms(u, term):
        spread(first.at[u], sems(u, 0), mx, side + my, (term[:, :half], term[:, half:]))

    def send_sums(u):
        landed(first.at[u], recv_sem.at[turn(u), 0])
        spread(second.at[u], sems(u, 1), side + mx, my, (total(first.at[u], side), total(first.at[u], 0)))

    def summed(u):
        landed(second.at[u], recv_sem.at[turn(u), 1])
        return jnp.concatenate([total(second.at[u], 0), total(second.at[u], side)], axis=1)

    def deal():
        slots = dealt.at[1]
        slots[me] = dealt[0, me]
        for peer in everyone:
            send(dealt.at[0, peer], slots.at[me], send_sem.at[2], deal_recv_sem.at[0], peer)

    def waited(slots, sem):
        rest = slots.at[pl.ds(0, side * side - 1)]
        pltpu.make_async_copy(rest, rest, sem).wait()

    def settle():
        slots, sums = dealt.at[1], dealt.at[2]
        waited(slots, deal_recv_sem.at[0])
        t = slots[0].astype(F32)
        for i in range(1, side * side):
            t = t + slots[i].astype(F32)
        sums[me] = t.astype(BF16)
        for peer in everyone:
            send(sums.at[me], sums.at[me], send_sem.at[3], deal_recv_sem.at[1], peer)

    def settled():
        sums = dealt.at[2]
        waited(sums, deal_recv_sem.at[1])
        return jnp.concatenate([sums[i].astype(F32) for i in range(side * side)], axis=1)

    def project(u, o):
        send_terms(u, dot(o.astype(BF16), wo_ref[...]))

    def middle(u):
        h = (x_ref[u].astype(F32) + summed(u)).astype(BF16)
        h_ref[u] = h
        b_ref[u] = scaled(h.astype(F32), gain_m_ref[...])

    def mlp(b):
        gate, up = dot(b, wg_ref[...]), dot(b, wu_ref[...])
        return dot((jax.nn.silu(gate) * up).astype(BF16), wd_ref[...])

    def finish(u, total):
        y_ref[u] = (h_ref[u].astype(F32) + total).astype(BF16)

    def step(u, carry):
        for c in (0, 1):
            score_half(u, c)
            refill(u, c)
        weigh()

        @pl.when(u == 0)
        def _():
            copies[len(early) - 1].wait()

        arrived(u, 2)
        part_o[...] = mixed(u, range(PART))
        refill(u, 2)
        arrived(u, 3)
        project(u, part_o[...] + mixed(u, range(PART, UNIT)))
        refill(u, 3)

        @pl.when(u > 0)
        def _():
            send_sums(u - 1)

        @pl.when((u > 1) & (u < units - 2))
        def _():
            middle(u - 2)

        return carry

    lax.fori_loop(0, units - 1, step, 0)

    e, f = units - 2, units - 1
    for c in (0, 1):
        score_half(f, c)
    weigh()
    arrived(f, 2)
    part_o[...] = mixed(f, range(PART))
    arrived(f, 3, (0,))
    part_o[...] += mixed(f, range(PART, UNIT), 0, cache // 2)
    arrived(f, 3, (1,))
    for copy in copies[len(early):]:
        copy.start()
    project(f, part_o[...] + mixed(f, range(PART, UNIT), cache // 2, cache))

    send_sums(e)
    middle(e - 2)
    middle(e - 1)
    for copy in copies[len(early):]:
        copy.wait()
    term = mlp(b_ref[pl.ds(0, e)].astype(F32).reshape(e * UNIT, d).astype(BF16))
    width = d // (side * side)
    for i in range(side * side):
        dealt[0, i] = term[:, i * width:(i + 1) * width].astype(BF16)
    send_sums(f)
    deal()
    middle(e)
    send_terms(units, mlp(b_ref[e]))
    middle(f)
    send_terms(units + 1, mlp(b_ref[f]))
    settle()
    send_sums(units)
    send_sums(units + 1)
    finish(e, summed(units))
    t = settled()
    for u in range(e):
        finish(u, t[u * UNIT:(u + 1) * UNIT])
    finish(f, summed(units + 1))

    others, rest = pl.ds(0, 2 * (side - 1)), pl.ds(0, side * side - 1)
    for sem, sent in enumerate((first.at[:, others], second.at[:, others], dealt.at[0, rest], dealt.at[2, rest])):
        pltpu.make_async_copy(sent, sent, send_sem.at[sem]).wait()


def turn_table(cache):
    half = HEAD // 2
    angle = (cache - 1) * float(THETA) ** (-np.arange(half) / half)
    cos, sin = np.cos(angle), np.sin(angle)
    table = np.zeros((8, HEAD), np.float32)
    table[0] = np.concatenate([cos, cos])
    table[1] = np.concatenate([-sin, sin])
    return table


def solution(mesh):
    devices = mesh.shape["tp"]
    side = int(devices**0.5)

    def step(x, k_cache, v_cache, gain_a, wq, wo, gain_m, w_gate, w_up, w_down):
        batch, cache = k_cache.shape[:2]
        d = x.shape[1]
        units = batch // UNIT
        hbm = pl.BlockSpec(memory_space=pltpu.HBM)
        operands = (
            x.reshape(units, UNIT, d), gain_a, gain_m, jnp.asarray(turn_table(cache)),
            wq, wo, w_gate, w_up, w_down, k_cache.reshape(batch * cache, HEAD), v_cache.reshape(batch * cache, HEAD),
        )
        operands = tuple(pltpu.with_memory_space_constraint(t, pltpu.HBM) for t in operands)
        buffers = pltpu.VMEM((units + 2, 2 * side, UNIT, d // 2), BF16)
        y = pl.pallas_call(
            functools.partial(layer, side, cache),
            name="layer",
            out_shape=jax.ShapeDtypeStruct((units, UNIT, d), BF16),
            in_specs=[hbm] * len(operands),
            out_specs=pl.BlockSpec(memory_space=pltpu.VMEM),
            scratch_shapes=[pltpu.VMEM(t.shape, t.dtype) for t in operands[:-2]] + [
                pltpu.VMEM((AHEAD * CHUNKS, PART * cache, HEAD), BF16),
                pltpu.VMEM((units, UNIT, UNIT * HEAD), BF16),
                pltpu.VMEM((UNIT, cache), F32),
                pltpu.VMEM((UNIT, cache), BF16),
                pltpu.VMEM((UNIT, HEAD), F32),
                pltpu.VMEM((units, UNIT, d), BF16),
                pltpu.VMEM((units, UNIT, d), BF16),
                buffers,
                buffers,
                pltpu.VMEM((3, devices, (units - 2) * UNIT, d // devices), BF16),
                pltpu.SemaphoreType.DMA((4,)),
                pltpu.SemaphoreType.DMA((AHEAD * (CHUNKS + 1),)),
                pltpu.SemaphoreType.DMA((4,)),
                pltpu.SemaphoreType.DMA((TURNS + 2, 2)),
                pltpu.SemaphoreType.DMA((2,)),
            ],
            compiler_params=pltpu.CompilerParams(collective_id=0, has_side_effects=True, vmem_limit_bytes=52 * 2**20),
        )(*operands)
        return y.reshape(batch, d)

    states, cache, columns, rows_of = P("dp", None), P("dp", None, "tp", None), P(None, "tp"), P("tp", None)
    return jax.shard_map(
        step,
        mesh=mesh,
        in_specs=(states, cache, cache, P(None), columns, rows_of, P(None), columns, columns, rows_of),
        out_specs=states,
        check_vma=False,
    )
```
